32 devices in a mesh: dp: 1, ep: 32 (over z, y, x, core).
Axes of the slice: x: 2, y: 2, z: 4, core: 2. Of those that a mesh axis runs over, the one named last changes fastest.
Arguments:
- tokens: bfloat16 [256, 1024], P(('dp', 'ep')), may hold values from -6 to 6
- expert_ids: int32 [256, 8], P(('dp', 'ep')), may hold values from 0 to 31, all different within a row; in each aligned block of 8 rows (0 to 7, 8 to 15, ...) at most 4 rows name the same one
- gate_quant: int32 [256, 8], P(('dp', 'ep')), may hold values from 1 to 1024
- bucket_ids: int32 [256], P(('dp', 'ep')), may hold values from 0 to 15
- bucket_counts: int32 [16], replicated, may hold values from 0 to 512
- gate_weight: bfloat16 [32, 1024, 384], P('ep', 'dp'), may hold values from -0.1875 to 0.1875
- up_weight: bfloat16 [32, 1024, 384], P('ep', 'dp'), may hold values from -0.1875 to 0.1875
- down_weight: bfloat16 [32, 384, 1024], P('ep', 'dp'), may hold values from -0.3125 to 0.3125
- cotangent: bfloat16 [256, 1024], P(('dp', 'ep')), may hold values from -6 to 6
Outputs:
- layer_out: bfloat16 [256, 1024], P(('dp', 'ep'))
- token_grad: bfloat16 [256, 1024], P(('dp', 'ep'))
- gate_grad: float32 [32, 1024, 384], P('ep', 'dp')
- up_grad: float32 [32, 1024, 384], P('ep', 'dp')
- down_grad: float32 [32, 384, 1024], P('ep', 'dp')
The draws below stay inside these ranges and needn't reach their ends.
Inputs may be any that keep to these rules, and one draw needn't show every extreme that they name: `expert_ids`: each row names 8 different experts. Among the 8 rows of one device no expert is named by more than 4 rows, and in every draw some expert is named by exactly 4 rows of some device.
All inputs are finite; a program needn't handle non-finite values.
Results may differ from the reference program's by a relative error of at most 0.0085.
Values may be sent and summed in bfloat16 or wider, within the bound.
No kernel may reach another device: no remote copies, remote signals or barrier semaphores. Data moves between devices by JAX's collectives and lax.ppermute only.
A program may use at most 64 MiB of HBM per device.

```python
import math
import jax
import jax.numpy as jnp
import numpy as np
from jax import lax

D = 1024
FF = 384
TOP = 8
BUCKETS = 16
TOK_DEV = 8
EXPERTS = 32
CAP = 4
TOKENS = 256
N_DP = 1
N_EP = 32


def touch_ends(values, rng, smallest, largest):
    place = [jax.random.randint(jax.random.fold_in(rng, axis), (), 0, length) for axis, length in enumerate(values.shape)]
    longest = values.shape.index(max(values.shape))
    next_to = place[:longest] + [(place[longest] + 1) % values.shape[longest]] + place[longest + 1:]
    return values.at[tuple(place)].set(smallest).at[tuple(next_to)].set(largest)


def level_of(key, dims, shards, least, largest):
    gain, own = 1.0, jax.random.fold_in(key, 6)
    for dim, parts in shards:
        heights = jnp.exp(jax.random.uniform(jax.random.fold_in(own, dim), (parts,), jnp.float32, least / len(shards), largest / len(shards)))
        gain = gain * jnp.repeat(heights, dims[dim] // parts).reshape([-1 if axis == dim else 1 for axis in range(len(dims))])
    return gain


def assign_block(own_key, own, number, rows, number_of, top, bound, skew):
    sequence = jax.random.permutation(own_key, number_of)
    heavy_load, ordinary = shares(number_of, rows * top, bound, skew, True), shares(number_of, rows * top, bound, skew, False)
    places = jnp.arange(number_of)

    def named(sizes, turn):
        used = int((sizes > 0).sum())
        fixed = max(1, used // 4)
        shifted = fixed + (places - fixed + turn * (used - fixed)) % max(1, number_of - fixed)
        return jnp.zeros((number_of,), jnp.int32).at[sequence[jnp.where(places < fixed, places, shifted)]].set(jnp.asarray(sizes, jnp.int32))

    sizes = jnp.where(number % 4 == 0, named(heavy_load, number // 4), named(ordinary, number - number // 4 - 1))
    mixed = jax.random.permutation(jax.random.fold_in(own, 3), number_of)
    donor, sink = mixed[0:number_of // 2 * 2:2], mixed[1:number_of // 2 * 2:2]
    room = jnp.minimum(sizes[donor] - 1, bound - sizes[sink]) // 2
    room = jnp.where((donor == sequence[0]) | (sink == sequence[0]) | (sizes[sink] == 0), 0, jnp.maximum(room, 0))
    shifted = jax.random.randint(jax.random.fold_in(own, 4), (number_of // 2,), 0, 1 << 20) % (room + 1)
    sizes = sizes.at[donor].add(-shifted).at[sink].add(shifted)
    items = jnp.searchsorted(jnp.cumsum(sizes), jnp.arange(rows * top), side="right").astype(jnp.int32)
    table = items.reshape(top, rows).T
    table = table[jax.random.permutation(jax.random.fold_in(own, 1), rows)]
    turn = jax.random.randint(jax.random.fold_in(own, 2), (rows, 1), 0, top)
    return jnp.take_along_axis(table, (jnp.arange(top)[None, :] + turn) % top, axis=1)


def shares(amount, total, bound, lean, full):
    weights = [(1 << 20) // math.isqrt(grade ** lean) + 1 for grade in range(1, amount + 1)]
    largest = bound if full else min(bound, max(-(-total // amount), total * weights[0] // sum(weights)))
    least = 1 if total - largest >= amount - 1 else 0
    counts, rest = [largest] + [least] * (amount - 1), total - largest - least * (amount - 1)
    while rest > 0:
        candidates = [i for i in range(1, amount) if counts[i] < largest] or [i for i in range(1, amount) if counts[i] < bound]
        whole, budget = sum([weights[i] for i in candidates]), rest
        for i in candidates:
            more = min(bound - counts[i], max(1, budget * weights[i] // whole), rest)
            counts[i] = counts[i] + more
            rest = rest - more
    return np.array(counts)


def gaussian(key, dims, width, bound, split=(), kind=jnp.bfloat16):
    loudness = level_of(key, dims, split, -0.22, 0.18) if split else 1.0
    entries = jax.random.normal(key, dims, jnp.float32) * width * loudness
    return jnp.minimum(jnp.maximum(entries, -bound), bound).astype(kind)


def setup_inputs(seed: int = 0) -> dict:
    key_of = jax.random.split(jax.random.key(seed), 10)
    tokens = gaussian(key_of[0], (TOKENS, D), 1.0, 6.0, ((0, 32),))
    expert_ids_keys = jax.random.split(jax.random.fold_in(key_of[1], 1), TOKENS // TOK_DEV)
    expert_ids_turns = jax.random.permutation(jax.random.fold_in(key_of[1], 3), TOKENS // TOK_DEV)
    expert_ids = jax.vmap(lambda own, number: assign_block(jax.random.fold_in(key_of[1], 2), own, number, TOK_DEV, EXPERTS, TOP, CAP, 2))(expert_ids_keys, expert_ids_turns).reshape((TOKENS, TOP))
    gate_quant = touch_ends(jax.random.randint(key_of[2], (TOKENS, TOP), 1, 1025), jax.random.fold_in(key_of[2], 1), 1, 1024).astype(jnp.int32)
    bucket_ids = touch_ends(jax.random.randint(key_of[3], (TOKENS,), 0, BUCKETS), jax.random.fold_in(key_of[3], 1), 0, BUCKETS - 1).astype(jnp.int32)
    bucket_counts = touch_ends(jax.random.randint(key_of[4], (BUCKETS,), 0, 513), jax.random.fold_in(key_of[4], 1), 0, 512).astype(jnp.int32)
    gate_weight = gaussian(key_of[5], (EXPERTS, D, FF), D ** -0.5, 0.1875, ((0, 32),))
    up_weight = gaussian(key_of[6], (EXPERTS, D, FF), D ** -0.5, 0.1875, ((0, 32),))
    down_weight = gaussian(key_of[7], (EXPERTS, FF, D), FF ** -0.5, 0.3125, ((0, 32),))
    cotangent = gaussian(key_of[8], (TOKENS, D), 1.0, 6.0, ((0, 32),))
    return {"tokens": tokens, "expert_ids": expert_ids, "gate_quant": gate_quant, "bucket_ids": bucket_ids, "bucket_counts": bucket_counts, "gate_weight": gate_weight, "up_weight": up_weight, "down_weight": down_weight, "cotangent": cotangent}


def silu_parts(pre_gate):
    sigmoid_val = jax.nn.sigmoid(pre_gate)
    return pre_gate * sigmoid_val, sigmoid_val * (1.0 + pre_gate * (1.0 - sigmoid_val))


def contract_rows(left_rows, right_rows):
    return lax.dot_general(left_rows, right_rows, (((0,), (0,)), ((), ())), preferred_element_type=jnp.float32)


def contract_cols(left_rows, right_rows):
    return lax.dot_general(left_rows, right_rows, (((1,), (1,)), ((), ())), preferred_element_type=jnp.float32)


def expert_forward(rows_in, gate_full, up_full, down_full):
    pre_gate = jnp.dot(rows_in, gate_full, preferred_element_type=jnp.float32)
    pre_up = jnp.dot(rows_in, up_full, preferred_element_type=jnp.float32)
    activation, derivative = silu_parts(pre_gate)
    hidden = (activation * pre_up).astype(jnp.bfloat16)
    expert_out = jnp.dot(hidden, down_full, preferred_element_type=jnp.float32).astype(jnp.bfloat16)
    return expert_out, (pre_up, activation, derivative, hidden)


def expert_backward(rows_in, scaled, saved, gate_full, up_full, down_full):
    pre_up, activation, derivative, hidden = saved
    hidden_grad = contract_cols(scaled, down_full)
    gate_pre = (hidden_grad * pre_up * derivative).astype(jnp.bfloat16)
    up_pre = (hidden_grad * activation).astype(jnp.bfloat16)
    slot_grad = (contract_cols(gate_pre, gate_full) + contract_cols(up_pre, up_full)).astype(jnp.bfloat16)
    return slot_grad, contract_rows(rows_in, gate_pre), contract_rows(rows_in, up_pre), contract_rows(hidden, scaled)


def slot_table(flat_ids, experts, slot_cap):
    total_pairs = flat_ids.shape[0]
    onehot = (flat_ids[:, None] == jnp.arange(experts, dtype=jnp.int32)[None, :]).astype(jnp.int32)
    before = jnp.cumsum(onehot, axis=0) - onehot
    position = jnp.sum(before * onehot, axis=1)
    slot_of = (flat_ids * slot_cap + position).astype(jnp.int32)
    lookup = jnp.full((experts * slot_cap,), total_pairs, jnp.int32)
    lookup = lookup.at[slot_of].set(jnp.arange(total_pairs, dtype=jnp.int32))
    return lookup, slot_of


def reference(tokens, expert_ids, gate_quant, bucket_ids, bucket_counts, gate_weight, up_weight, down_weight, cotangent):
    experts = gate_weight.shape[0]
    top_count = expert_ids.shape[1]
    group_size = N_EP * TOK_DEV
    slot_cap = N_EP * CAP
    model_width = tokens.shape[1]
    gate_share = gate_quant.astype(jnp.float32) / 1024.0
    token_scale = 64.0 / (64.0 + bucket_counts[bucket_ids].astype(jnp.float32))
    scaled_share = gate_share * token_scale[:, None]
    out_parts = []
    grad_parts = []
    totals = None
    for group_idx in range(N_DP):
        first_row = group_idx * group_size
        group_tokens = tokens[first_row:first_row + group_size]
        group_cot = cotangent[first_row:first_row + group_size]
        flat_ids = expert_ids[first_row:first_row + group_size].reshape(-1)
        gate_flat = gate_share[first_row:first_row + group_size].reshape(-1)
        scaled_flat = scaled_share[first_row:first_row + group_size].reshape(-1)
        lookup, slot_of = slot_table(flat_ids, experts, slot_cap)
        total_pairs = flat_ids.shape[0]

        def per_expert(running, expert_item):
            out_acc, grad_acc = running
            pair_index, gate_full, up_full, down_full = expert_item
            is_live = pair_index < total_pairs
            safe_index = jnp.where(is_live, pair_index, 0).astype(jnp.int32)
            source_row = (safe_index // top_count).astype(jnp.int32)
            rows_in = jnp.where(is_live[:, None], group_tokens[source_row], jnp.zeros((), jnp.bfloat16)).astype(jnp.bfloat16)
            gate_slot = jnp.where(is_live, gate_flat[safe_index], jnp.zeros((), jnp.float32))
            scale_slot = jnp.where(is_live, scaled_flat[safe_index], jnp.zeros((), jnp.float32))
            scaled = (scale_slot[:, None] * group_cot[source_row].astype(jnp.float32)).astype(jnp.bfloat16)
            expert_out, saved = expert_forward(rows_in, gate_full, up_full, down_full)
            slot_grad, grad_gate, grad_up, grad_down = expert_backward(rows_in, scaled, saved, gate_full, up_full, down_full)
            out_acc = out_acc.at[source_row].add(gate_slot[:, None] * expert_out.astype(jnp.float32))
            grad_acc = grad_acc.at[source_row].add(jnp.where(is_live[:, None], slot_grad.astype(jnp.float32), jnp.zeros((), jnp.float32)))
            return (out_acc, grad_acc), (grad_gate.astype(jnp.bfloat16), grad_up.astype(jnp.bfloat16), grad_down.astype(jnp.bfloat16))

        start_acc = (jnp.zeros((group_size, model_width), jnp.float32), jnp.zeros((group_size, model_width), jnp.float32))
        stacked = (lookup.reshape(experts, slot_cap), gate_weight, up_weight, down_weight)
        (out_acc, grad_acc), partials = lax.scan(per_expert, start_acc, stacked)
        out_parts.append(out_acc.astype(jnp.bfloat16))
        grad_parts.append(grad_acc.astype(jnp.bfloat16))
        widened = tuple(part.astype(jnp.float32) for part in partials)
        if totals is None:
            totals = widened
        else:
            totals = tuple(acc + part for acc, part in zip(totals, widened))
    layer_out = jnp.concatenate(out_parts, axis=0)
    token_grad = jnp.concatenate(grad_parts, axis=0)
    return (layer_out, token_grad, totals[0], totals[1], totals[2])
```

```python
import jax
import jax.numpy as jnp
from jax import lax
from jax.sharding import PartitionSpec as P

LANES = 128


def silu_parts(pre_gate):
    sigmoid_val = jax.nn.sigmoid(pre_gate)
    return (pre_gate * sigmoid_val, sigmoid_val * (1.0 + pre_gate * (1.0 - sigmoid_val)))


def contract_rows(left_rows, right_rows):
    return lax.dot_general(
        left_rows, right_rows, (((0,), (0,)), ((), ())), preferred_element_type=jnp.float32
    )


def contract_cols(left_rows, right_rows):
    return lax.dot_general(
        left_rows, right_rows, (((1,), (1,)), ((), ())), preferred_element_type=jnp.float32
    )


def stages(devices):
    out = [(1, 2)]
    stride = 2
    while stride < devices:
        radix = min(4, devices // stride)
        out.append((stride, radix))
        stride *= radix
    return out[::-1]


def send_to(rows, devices, offset):
    return lax.ppermute(rows, "ep", [(dev, dev ^ offset) for dev in range(devices)])


def gather_all(rows, devices):
    held = rows[None]
    for stride, radix in stages(devices):
        parts = [held] + [send_to(held, devices, stride * j) for j in range(1, radix)]
        held = jnp.concatenate(parts, axis=0)
    return held


def reduce_all(blocks, devices):
    held = blocks
    for stride, radix in stages(devices)[::-1]:
        held = held.reshape(radix, -1, *held.shape[1:])
        total = held[0]
        for j in range(1, radix):
            total = total + send_to(held[j].astype(jnp.bfloat16), devices, stride * j).astype(
                jnp.float32
            )
        held = total
    return held[0]


def per_device(
    tokens,
    expert_ids,
    gate_quant,
    bucket_ids,
    bucket_counts,
    gate_weight,
    up_weight,
    down_weight,
    cotangent,
):
    devices = lax.axis_size("ep")
    tok_rows, top_count = expert_ids.shape
    width = tokens.shape[1]
    routing = jnp.concatenate(
        [expert_ids, gate_quant >> 5, gate_quant & 31, bucket_ids[:, None]], axis=1
    ).astype(jnp.bfloat16)
    routing = jnp.pad(routing, ((0, 0), (0, LANES - routing.shape[1])))
    payload = jnp.concatenate([tokens, cotangent, routing], axis=1)
    every = gather_all(payload, devices).reshape(devices * tok_rows, -1)
    rows_in = every[:, :width]
    cot_rows = every[:, width : 2 * width].astype(jnp.float32)
    routing = every[:, 2 * width :].astype(jnp.float32)
    mine = routing[:, :top_count] == lax.axis_index("ep").astype(jnp.float32)
    quant = routing[:, top_count : 2 * top_count] * 32.0 + routing[:, 2 * top_count : 3 * top_count]
    share = jnp.sum(jnp.where(mine, quant, 0.0), axis=1, keepdims=True) / 1024.0
    buckets = jnp.arange(bucket_counts.shape[0], dtype=jnp.int32).astype(jnp.float32)
    bucket_match = routing[:, 3 * top_count : 3 * top_count + 1] == buckets[None, :]
    count_of = jnp.sum(
        jnp.where(bucket_match, bucket_counts.astype(jnp.float32)[None, :], 0.0),
        axis=1,
        keepdims=True,
    )
    scale = share * (64.0 / (64.0 + count_of))
    gate_full, up_full, down_full = (
        lax.all_gather(gate_weight, "dp", axis=1, tiled=True)[0],
        lax.all_gather(up_weight, "dp", axis=1, tiled=True)[0],
        lax.all_gather(down_weight, "dp", axis=1, tiled=True)[0],
    )
    pre_gate = jnp.dot(rows_in, gate_full, preferred_element_type=jnp.float32)
    pre_up = jnp.dot(rows_in, up_full, preferred_element_type=jnp.float32)
    activation, derivative = silu_parts(pre_gate)
    hidden = (activation * pre_up).astype(jnp.bfloat16)
    expert_out = jnp.dot(hidden, down_full, preferred_element_type=jnp.float32)
    scaled = (scale * cot_rows).astype(jnp.bfloat16)
    hidden_grad = contract_cols(scaled, down_full)
    gate_pre = (hidden_grad * pre_up * derivative).astype(jnp.bfloat16)
    up_pre = (hidden_grad * activation).astype(jnp.bfloat16)
    slot_grad = contract_cols(gate_pre, gate_full) + contract_cols(up_pre, up_full)
    terms = jnp.concatenate([share * expert_out, slot_grad], axis=1)
    total = reduce_all(terms.reshape(devices, tok_rows, 2 * width), devices).astype(jnp.bfloat16)
    layer_out, token_grad = total[:, :width], total[:, width:]
    summed = [
        lax.psum_scatter(
            grad[None].astype(jnp.bfloat16), "dp", scatter_dimension=1, tiled=True
        ).astype(jnp.float32)
        for grad in (
            contract_rows(rows_in, gate_pre),
            contract_rows(rows_in, up_pre),
            contract_rows(hidden, scaled),
        )
    ]
    return (layer_out, token_grad, summed[0], summed[1], summed[2])


def solution(mesh):
    rows = P(("dp", "ep"), None)
    weights = P("ep", "dp", None)
    return jax.shard_map(
        per_device,
        mesh=mesh,
        in_specs=(rows, rows, rows, P(("dp", "ep")), P(), weights, weights, weights, rows),
        out_specs=(rows, rows, weights, weights, weights),
        check_vma=False,
    )
```

```python
import functools

import jax
import jax.numpy as jnp
from jax import lax
from jax.experimental import pallas as pl
from jax.experimental.pallas import tpu as pltpu
from jax.sharding import PartitionSpec as P

LANES = 128
VMEM_LIMIT = 24 * 1024 * 1024


def silu_parts(pre_gate):
    sigmoid_val = jax.nn.sigmoid(pre_gate)
    return (pre_gate * sigmoid_val, sigmoid_val * (1.0 + pre_gate * (1.0 - sigmoid_val)))


def contract_rows(left_rows, right_rows):
    return lax.dot_general(
        left_rows, right_rows, (((0,), (0,)), ((), ())), preferred_element_type=jnp.float32
    )


def contract_cols(left_rows, right_rows):
    return lax.dot_general(
        left_rows, right_rows, (((1,), (1,)), ((), ())), preferred_element_type=jnp.float32
    )


def wide_stages(devices):
    out = []
    stride = 8
    while stride < devices:
        radix = min(4, devices // stride)
        out.append((stride, radix))
        stride *= radix
    return out[::-1]


def send_to(rows, devices, offset):
    return lax.ppermute(rows, "ep", [(dev, dev ^ offset) for dev in range(devices)])


def vmem_specs(count):
    return [pl.BlockSpec(memory_space=pltpu.VMEM)] * count


def smem_spec():
    return pl.BlockSpec(memory_space=pltpu.SMEM)


def call(kernel, out_shape, in_specs, flops=0, moved=0, transcendentals=0, **kwargs):
    several = isinstance(out_shape, (list, tuple))
    return pl.pallas_call(
        kernel,
        out_shape=out_shape,
        in_specs=in_specs,
        out_specs=vmem_specs(len(out_shape)) if several else vmem_specs(1)[0],
        compiler_params=pltpu.CompilerParams(vmem_limit_bytes=VMEM_LIMIT),
        cost_estimate=pl.CostEstimate(
            flops=flops, bytes_accessed=moved, transcendentals=transcendentals
        ),
        **kwargs,
    )


def payload_kernel(
    bucket_ref,
    counts_ref,
    tokens_ref,
    ids_ref,
    quant_ref,
    cot_ref,
    out_ref,
    bucket_buf,
    counts_buf,
    tokens_buf,
    ids_buf,
    quant_buf,
    cot_buf,
    sems,
):
    rows, width = tokens_ref.shape
    pairs = (
        (bucket_ref, bucket_buf),
        (counts_ref, counts_buf),
        (ids_ref, ids_buf),
        (quant_ref, quant_buf),
        (tokens_ref, tokens_buf),
        (cot_ref, cot_buf),
    )
    copies = [pltpu.make_async_copy(src, dst, sems.at[i]) for i, (src, dst) in enumerate(pairs)]
    for copy in copies:
        copy.start()
    for copy in copies:
        copy.wait()
    row = lax.broadcasted_iota(jnp.int32, (rows, 1), 0)
    count = jnp.zeros((rows, 1), jnp.int32)
    for r in range(rows):
        count = jnp.where(row == r, counts_buf[bucket_buf[r]], count)
    quant = quant_buf[...]
    routing = jnp.concatenate(
        [ids_buf[...], quant >> 5, quant & 31, count >> 5, count & 31], axis=1
    ).astype(jnp.float32)
    routing = jnp.concatenate(
        [routing, jnp.zeros((rows, LANES - routing.shape[1]), jnp.float32)], axis=1
    )
    out_ref[:, :width] = tokens_buf[...]
    out_ref[:, width : 2 * width] = cot_buf[...]
    out_ref[:, 2 * width :] = routing.astype(jnp.bfloat16)


def fetch_kernel(count, *refs):
    sources, targets, sems = refs[:count], refs[count : 2 * count], refs[-1]
    copies = [
        pltpu.make_async_copy(src, dst, sems.at[i])
        for i, (src, dst) in enumerate(zip(sources, targets))
    ]
    for copy in copies:
        copy.start()
    for copy in copies:
        copy.wait()


def in_hbm(arrays):
    return [pltpu.with_memory_space_constraint(array, pltpu.HBM) for array in arrays]


def fetch(arrays):
    moved = sum(2 * array.size for array in arrays)
    return call(
        functools.partial(fetch_kernel, len(arrays)),
        [jax.ShapeDtypeStruct(array.shape, array.dtype) for array in arrays],
        [pl.BlockSpec(memory_space=pltpu.HBM)] * len(arrays),
        flops=1000 * moved,
        moved=moved,
        scratch_shapes=[pltpu.SemaphoreType.DMA((len(arrays),))],
    )(*in_hbm(arrays))


def join_kernel(*refs):
    out_ref = refs[-1]
    start = 0
    for ref in refs[:-1]:
        out_ref[start : start + ref.shape[0], :] = ref[...]
        start += ref.shape[0]


def join(pieces):
    rows = sum(piece.shape[0] for piece in pieces)
    return call(
        join_kernel,
        jax.ShapeDtypeStruct((rows, pieces[0].shape[1]), pieces[0].dtype),
        vmem_specs(len(pieces)),
        flops=rows * pieces[0].shape[1],
        moved=4 * rows * pieces[0].shape[1],
    )(*pieces)


def expert_kernel(pieces, top_count, *refs):
    me_ref, gate_ref, up_ref, down_ref = refs[:4]
    piece_refs = refs[4 : 4 + pieces]
    rows_ref, scaled_ref, hidden_ref, gate_pre_ref, up_pre_ref = refs[4 + pieces : 9 + pieces]
    term_refs = refs[9 + pieces :]
    width = gate_ref.shape[0]
    rows_in = jnp.concatenate([ref[:, :width] for ref in piece_refs], axis=0)
    routing = jnp.concatenate([ref[:, 2 * width :] for ref in piece_refs], axis=0).astype(
        jnp.float32
    )
    me = me_ref[0].astype(jnp.float32)
    mine = routing[:, :top_count] == me
    quant = routing[:, top_count : 2 * top_count] * 32.0 + routing[:, 2 * top_count : 3 * top_count]
    share = jnp.sum(jnp.where(mine, quant, 0.0), axis=1, keepdims=True) / 1024.0
    count = (
        routing[:, 3 * top_count : 3 * top_count + 1] * 32.0
        + routing[:, 3 * top_count + 1 : 3 * top_count + 2]
    )
    scale = share * (64.0 / (64.0 + count))
    cot_rows = jnp.concatenate([ref[:, width : 2 * width] for ref in piece_refs], axis=0)
    scaled = (scale * cot_rows.astype(jnp.float32)).astype(jnp.bfloat16)
    rows_ref[...] = rows_in
    scaled_ref[...] = scaled
    pre_gate = jnp.dot(rows_in, gate_ref[...], preferred_element_type=jnp.float32)
    pre_up = jnp.dot(rows_in, up_ref[...], preferred_element_type=jnp.float32)
    hidden_grad = contract_cols(scaled, down_ref[...])
    activation, derivative = silu_parts(pre_gate)
    hidden = (activation * pre_up).astype(jnp.bfloat16)
    gate_pre = (hidden_grad * pre_up * derivative).astype(jnp.bfloat16)
    up_pre = (hidden_grad * activation).astype(jnp.bfloat16)
    hidden_ref[...] = hidden
    gate_pre_ref[...] = gate_pre
    up_pre_ref[...] = up_pre
    out = share * jnp.dot(hidden, down_ref[...], preferred_element_type=jnp.float32)
    start = 0
    for ref in term_refs:
        ref[:, :width] = out[start : start + ref.shape[0]].astype(ref.dtype)
        start += ref.shape[0]
    grad = contract_cols(gate_pre, gate_ref[...]) + contract_cols(up_pre, up_ref[...])
    start = 0
    for ref in term_refs:
        ref[:, width:] = grad[start : start + ref.shape[0]].astype(ref.dtype)
        start += ref.shape[0]


def per_device(
    tokens,
    expert_ids,
    gate_quant,
    bucket_ids,
    bucket_counts,
    gate_weight,
    up_weight,
    down_weight,
    cotangent,
):
    devices = lax.axis_size("ep")
    tok_rows, top_count = expert_ids.shape
    width = tokens.shape[1]
    bf16, f32 = jnp.bfloat16, jnp.float32
    me = lax.axis_index("ep").reshape(1)
    gate_full, up_full, down_full = (
        lax.all_gather(gate_weight, "dp", axis=1, tiled=True)[0],
        lax.all_gather(up_weight, "dp", axis=1, tiled=True)[0],
        lax.all_gather(down_weight, "dp", axis=1, tiled=True)[0],
    )
    hidden_width = gate_full.shape[1]
    gate_near, up_near, down_near = fetch([gate_full, up_full, down_full])

    held = call(
        payload_kernel,
        jax.ShapeDtypeStruct((tok_rows, 2 * width + LANES), bf16),
        [pl.BlockSpec(memory_space=pltpu.HBM)] * 6,
        flops=tok_rows * width,
        moved=8 * tok_rows * width,
        scratch_shapes=[
            pltpu.SMEM(bucket_ids.shape, jnp.int32),
            pltpu.SMEM(bucket_counts.shape, jnp.int32),
            pltpu.VMEM(tokens.shape, bf16),
            pltpu.VMEM(expert_ids.shape, jnp.int32),
            pltpu.VMEM(gate_quant.shape, jnp.int32),
            pltpu.VMEM(cotangent.shape, bf16),
            pltpu.SemaphoreType.DMA((6,)),
        ],
    )(*in_hbm([bucket_ids, bucket_counts, tokens, expert_ids, gate_quant, cotangent]))
    for stride, radix in wide_stages(devices):
        held = join([held] + [send_to(held, devices, stride * j) for j in range(1, radix)])
    near = [held] + [send_to(held, devices, 2 * j) for j in range(1, 4)]
    far = [send_to(piece, devices, 1) for piece in near]

    pieces = near + far
    block = held.shape[0]
    rows = block * len(pieces)
    wide = jax.ShapeDtypeStruct((rows, width), bf16)
    slim = jax.ShapeDtypeStruct((rows, hidden_width), bf16)
    outs = call(
        functools.partial(expert_kernel, len(pieces), top_count),
        [wide, wide, slim, slim, slim]
        + [jax.ShapeDtypeStruct((block, 2 * width), f32)] * 4
        + [jax.ShapeDtypeStruct((block, 2 * width), bf16)] * 4,
        [smem_spec(), *vmem_specs(3 + len(pieces))],
        flops=12 * rows * width * hidden_width,
        moved=2 * (3 * width * hidden_width + 8 * rows * width),
        transcendentals=rows * hidden_width,
    )(me, gate_near, up_near, down_near, *pieces)
    rows_in, scaled, hidden, gate_pre, up_pre = outs[:5]
    own, other = outs[5:9], outs[9:]

    sums = [None] * 4
    for j in (3, 1, 2, 0):
        sums[j] = own[j] + send_to(other[j], devices, 1).astype(f32)
    total = sums[0]
    for j in (3, 1, 2):
        total = total + send_to(sums[j].astype(bf16), devices, 2 * j).astype(f32)
    for stride, radix in wide_stages(devices)[::-1]:
        blocks = total.reshape(radix, -1, 2 * width)
        total = blocks[0]
        for j in range(1, radix):
            total = total + send_to(blocks[j].astype(bf16), devices, stride * j).astype(f32)
    layer_out, token_grad = total[:, :width].astype(bf16), total[:, width:].astype(bf16)
    summed = [
        lax.psum_scatter(grad[None].astype(bf16), "dp", scatter_dimension=1, tiled=True).astype(f32)
        for grad in (
            contract_rows(rows_in, gate_pre),
            contract_rows(rows_in, up_pre),
            contract_rows(hidden, scaled),
        )
    ]
    return (layer_out, token_grad, summed[0], summed[1], summed[2])


def solution(mesh):
    rows = P(("dp", "ep"), None)
    weights = P("ep", "dp", None)
    return jax.shard_map(
        per_device,
        mesh=mesh,
        in_specs=(rows, rows, rows, P(("dp", "ep")), P(), weights, weights, weights, rows),
        out_specs=(rows, rows, weights, weights, weights),
        check_vma=False,
    )
```
